128 devices in a mesh: row: 2 (over core), col: 64 (over z, y, x).
Axes of the slice: x: 4, y: 4, z: 4, core: 2. Of those that a mesh axis runs over, the one named last changes fastest.
Arguments:
- v_panels: float32 [6144, 6144], P('row', 'col')
- t_factors: float32 [192, 32, 32], P('col')
- z_vecs: float32 [6144, 4096], P(None, ('row', 'col'))
Outputs:
- output: float32 [6144, 4096], P(None, ('row', 'col'))
All inputs are finite; a program needn't handle non-finite values.
Results may differ from the reference program's by a relative error of at most 0.001.
Values sent between devices are 32-bit elements.
A program may use at most 1 GiB of HBM per device.

```python
import jax
import jax.numpy as jnp
from jax import lax

N = 6144
BLOCK = 32
K_DEV = 32
ROW_DEV = 2
COL_DEV = 64

NPANEL = N // BLOCK
M_LOC = NPANEL // COL_DEV
K_COLS = K_DEV * ROW_DEV * COL_DEV


def build_inputs(raw_vals, z_vecs):
    row_nat = jnp.arange(N)[:, None, None]
    diag_row = (jnp.arange(NPANEL) * BLOCK)[None, :, None] + jnp.arange(BLOCK)[None, None, :]
    v_nat = jnp.where(row_nat > diag_row, raw_vals, jnp.where(row_nat == diag_row, 1.0, 0.0)).astype(raw_vals.dtype)
    gram = jnp.einsum("nmb,nmc->mbc", v_nat, v_nat, precision=lax.Precision.HIGHEST)
    half_diag = 0.5 * jnp.diagonal(gram, axis1=1, axis2=2)
    t_inverse = jnp.triu(gram, 1) + jnp.eye(BLOCK, dtype=raw_vals.dtype) * half_diag[:, None, :]
    t_nat = jnp.triu(jnp.linalg.inv(t_inverse))
    v_cols = v_nat.reshape(N, M_LOC, COL_DEV, BLOCK).transpose(0, 2, 1, 3).reshape(N, N)
    v_store = v_cols.reshape(NPANEL // ROW_DEV, ROW_DEV, BLOCK, N).transpose(1, 0, 2, 3).reshape(N, N)
    t_store = t_nat.reshape(M_LOC, COL_DEV, BLOCK, BLOCK).transpose(1, 0, 2, 3).reshape(NPANEL, BLOCK, BLOCK)
    return {"v_panels": v_store, "t_factors": t_store, "z_vecs": z_vecs}


def setup_inputs(seed: int = 0) -> dict:
    base_key = jax.random.key(seed)
    key_v, key_z = jax.random.split(base_key)
    raw_vals = jax.random.normal(key_v, (N, NPANEL, BLOCK), jnp.float32)
    z_vecs = jax.random.normal(key_z, (N, K_COLS), jnp.float32)
    return build_inputs(raw_vals, z_vecs)


def reference(v_panels, t_factors, z_vecs):
    def apply_panel(x_cur, panel_idx):
        store_slot = (panel_idx % COL_DEV) * M_LOC + panel_idx // COL_DEV
        v_blk = lax.dynamic_slice_in_dim(v_panels, store_slot * BLOCK, BLOCK, axis=1)
        t_blk = lax.dynamic_index_in_dim(t_factors, store_slot, axis=0, keepdims=False)
        w_blk = jnp.dot(v_blk.T, x_cur, precision=lax.Precision.HIGHEST, preferred_element_type=jnp.float32)
        y_blk = jnp.dot(t_blk, w_blk, precision=lax.Precision.HIGHEST, preferred_element_type=jnp.float32)
        x_new = x_cur - jnp.dot(v_blk, y_blk, precision=lax.Precision.HIGHEST, preferred_element_type=jnp.float32)
        return x_new, None

    x_out, _ = lax.scan(apply_panel, z_vecs, jnp.arange(NPANEL - 1, -1, -1))
    return x_out
```

```python
import functools

import jax
import jax.numpy as jnp
from jax import lax
from jax.experimental import pallas as pl
from jax.experimental.pallas import tpu as pltpu
from jax.sharding import PartitionSpec as P

F32 = jnp.float32
BF16 = jnp.bfloat16
MESH_ID = pl.DeviceIdType.MESH
NT = (((1,), (1,)), ((), ()))
NN = (((1,), (0,)), ((), ()))

GROUPS = 24
T_UNITS = 8
ROUNDS = 5
UNITS = T_UNITS + GROUPS * (GROUPS + 1) // 2
ROUND_GROUPS = ((23, 14), (13, 9), (8, 6), (5, 3), (2, 0))
COLORS = ((0, 88, (2, 1, 0)), (88, 88, (1, 0, 2)), (176, 80, (0, 2, 1)))
PLUS_PART = 1


def split3(a):
    a1 = a.astype(BF16)
    r1 = a - a1.astype(F32)
    a2 = r1.astype(BF16)
    a3 = (r1 - a2.astype(F32)).astype(BF16)
    return a1, a2, a3


def dot(a, b, dims):
    return lax.dot_general(a, b, dims, preferred_element_type=F32)


def dot6(a, b, dims):
    a1, a2, a3 = a
    b1, b2, b3 = b
    m = a1.shape[0]
    p1 = dot(jnp.concatenate([a1, a2, a3], axis=0), b1, dims)
    p2 = dot(jnp.concatenate([a1, a2], axis=0), b2, dims)
    p3 = dot(a1, b3, dims)
    low = p1[2 * m:] + p2[m:] + p3
    mid = p1[m:2 * m] + p2[:m]
    return p1[:m] + (mid + low)


def first_unit(k):
    return T_UNITS + (23 - k) * (24 - k) // 2


def kernel(vt_ref, tp_ref, zt_ref, out_ref, units, x_ref, v1_ref, v2_ref, v3_ref,
           acc_w, acc_g, acc_s, part, peer, a2a_send, a2a_recv, z_sem, ag_send, ag_recv, px_send, px_recv):
    row = lax.axis_index("row")
    col = lax.axis_index("col")
    coord = (col // 16, (col // 4) % 4, col % 4)
    oct_id = col // 8
    lane_row = pl.multiple_of(32 * (col % 8), 32)
    other = 1 - row

    def unit_at(i):
        return units.at[i // 64, (i // 16) % 4, (i // 4) % 4, i % 4]

    my_cols = pl.ds(pl.multiple_of(32 * row, 32), 32)
    z_keep = pltpu.make_async_copy(zt_ref.at[row], x_ref.at[:, my_cols, :], z_sem.at[0])
    z_send = pltpu.make_async_remote_copy(
        src_ref=zt_ref.at[other], dst_ref=x_ref.at[:, my_cols, :],
        send_sem=z_sem.at[1], recv_sem=z_sem.at[2],
        device_id={"row": other}, device_id_type=MESH_ID)
    z_keep.start()
    z_send.start()

    def place(src, i, sem):
        dst = unit_at(i).at[pl.ds(lane_row, 32), :]
        owner = i % 64

        @pl.when(owner == col)
        def _():
            pltpu.make_async_copy(src, dst, a2a_recv.at[i // 64]).start()

        @pl.when(owner != col)
        def _():
            pltpu.make_async_remote_copy(
                src_ref=src, dst_ref=dst, send_sem=sem, recv_sem=a2a_recv.at[i // 64],
                device_id={"col": owner}, device_id_type=MESH_ID).start()

    def place_done(src, i, sem):
        @pl.when(i % 64 != col)
        def _():
            pltpu.make_async_remote_copy(
                src_ref=src, dst_ref=unit_at(i).at[pl.ds(lane_row, 32), :],
                send_sem=sem, recv_sem=a2a_recv.at[i // 64],
                device_id={"col": i % 64}, device_id_type=MESH_ID).wait_send()

    def each_block(fn):
        fn(tp_ref, oct_id, a2a_send.at[3, 0])
        for t in (2, 1, 0):
            k = 8 * t + oct_id

            def one(b, carry):
                fn(vt_ref.at[t, b], first_unit(k) + b - k, a2a_send.at[t, b])
                return carry

            lax.fori_loop(k, GROUPS, one, 0)

    each_block(place)

    def wait_own_unit(r):
        def go():
            mine = unit_at(64 * r + col)
            pltpu.make_async_copy(mine, mine, a2a_recv.at[r]).wait()

        if 64 * (r + 1) <= UNITS:
            go()
        else:
            pl.when(64 * r + col < UNITS)(go)

    def block(r, c, free, fixed):
        lo, n, _ = COLORS[c]
        sel = []
        for ax in range(3):
            if ax in fixed:
                sel.append(fixed[ax])
            elif ax in free:
                sel.append(free[ax])
            else:
                sel.append(coord[ax])
        return units.at[(r, *sel, pl.ds(lo, n), slice(None))]

    def hop(r, c, n, ax, d, free, fixed):
        ref = block(r, c, free, fixed)
        tgt = [coord[0], coord[1], coord[2]]
        tgt[ax] = (coord[ax] + d) % 4
        return pltpu.make_async_remote_copy(
            src_ref=ref, dst_ref=ref, send_sem=ag_send.at[r, c, n], recv_sem=ag_recv.at[r, c, n],
            device_id={"col": 16 * tgt[0] + 4 * tgt[1] + tgt[2]}, device_id_type=MESH_ID)

    FULL = slice(None)

    def hops(r, c, phase, incoming):
        a1, a2, a3 = COLORS[c][2]
        if phase == 0:
            spec = [(0, a1, 1, {}, {}), (1, a1, 3, {}, {}), (2, a1, 2, {}, {})]
        elif phase == 1:
            spec = [(3 + i, a2, d, {a1: FULL}, {}) for i, d in enumerate((1, 3, 2))]
        elif phase == 2:
            spec = [(6 + i, a3, d, {a1: FULL, a2: FULL}, {}) for i, d in enumerate((1, 3))]
        else:
            o, f = min(a1, a2), max(a1, a2)
            spec = []
            for i, d, part_sl in ((8, 1, pl.ds(0, PLUS_PART)), (9, 3, pl.ds(PLUS_PART, 4 - PLUS_PART))):
                frm = (coord[a3] - d) % 4
                spec.append((i, a3, d, {o: part_sl, f: FULL}, {a3: frm}))
        out = []
        for n, ax, d, free, fixed in spec:
            if incoming:
                fixed = dict(fixed)
                fixed[ax] = (coord[ax] - d) % 4 if phase < 3 else (coord[ax] + 2) % 4
            out.append(hop(r, c, n, ax, d, free, fixed))
        return out

    def start(r, phase):
        for c in range(3):
            for h in hops(r, c, phase, False):
                h.start()

    def arrive(r, phase):
        for c in range(3):
            for h in hops(r, c, phase, True):
                h.wait_recv()

    ri = lax.broadcasted_iota(jnp.int32, (256, 256), 0) // 32
    ci = lax.broadcasted_iota(jnp.int32, (256, 256), 1) // 32

    def group(k, carry):
        base = first_unit(k)
        slot = k % 2
        acc_w[...] = jnp.zeros_like(acc_w)
        acc_g[...] = jnp.zeros_like(acc_g)
        acc_s[...] = jnp.zeros_like(acc_s)

        def inner(p, c2):
            i0 = base + jnp.maximum(2 * p, k) - k
            lo = unit_at(i0)[...]
            lo = jnp.where(2 * p >= k, lo, 0.0)
            hi = unit_at(base + 2 * p + 1 - k)[...]
            v1, v2, v3 = split3(jnp.concatenate([lo, hi], axis=1))
            v1_ref[p] = v1
            v2_ref[p] = v2
            v3_ref[p] = v3
            x1, x2, x3 = split3(x_ref[p])
            p1 = dot(jnp.concatenate([x1, x2, x3, v1, v2, v3], axis=0), v1, NT)
            p2 = dot(jnp.concatenate([x1, x2, v2], axis=0), v2, NT)
            p3 = dot(x1, v3, NT)
            acc_w[...] += p1[:64] + ((p1[64:128] + p2[:64]) + (p1[128:192] + p2[64:128] + p3))
            acc_g[...] += p1[192:448] + p2[128:384]
            acc_s[...] += p1[448:704] + p1[704:960]
            return c2

        lax.fori_loop(k // 2, 12, inner, 0)
        s = acc_s[...]
        part[slot, 0:64] = acc_w[...]
        part[slot, 64:320] = acc_g[...] + (s + s.T)
        swap = pltpu.make_async_remote_copy(
            src_ref=part.at[slot], dst_ref=peer.at[slot], send_sem=px_send.at[slot], recv_sem=px_recv.at[slot],
            device_id={"row": other}, device_id_type=MESH_ID)
        swap.start()
        swap.wait()
        wt = part[slot, 0:64] + peer[slot, 0:64]
        gram = part[slot, 64:320] + peer[slot, 64:320]

        tsel = unit_at(k % 8)[...]
        lane = lax.broadcasted_iota(jnp.int32, (256, 128), 1) // 32
        tm = jnp.where(lane == k // 8, tsel, 0.0)
        tm = tm + pltpu.roll(tm, 32, 1)
        tm = tm + pltpu.roll(tm, 64, 1)
        tf = jnp.where(ri == ci, jnp.concatenate([tm, tm], axis=1), 0.0)
        for lvl in (1, 2, 4):
            off = (ri // (2 * lvl) == ci // (2 * lvl)) & (ri // lvl < ci // lvl)
            ts = split3(tf)
            mid = dot6(split3(jnp.where(off, gram, 0.0)), ts, NN)
            tf = tf - dot6(ts, split3(mid), NN)
        y1, y2, y3 = split3(dot6(split3(wt), split3(tf), NT))
        y12 = jnp.concatenate([y1, y2], axis=0)
        y123 = jnp.concatenate([y1, y2, y3], axis=0)

        def update(p, c2):
            p1 = dot(y123, v1_ref[p], NN)
            p2 = dot(y12, v2_ref[p], NN)
            p3 = dot(y1, v3_ref[p], NN)
            x_ref[p] = x_ref[p] - (p1[:64] + ((p1[64:128] + p2[:64]) + (p1[128:192] + p2[64:128] + p3)))
            return c2

        lax.fori_loop(k // 2, 12, update, 0)
        return carry

    z_keep.wait()
    z_send.wait()
    for step in range(ROUNDS + 4):
        r = step - 3
        if 0 <= r < ROUNDS:
            arrive(r, 2)
            start(r, 3)
        r = step - 2
        if 0 <= r < ROUNDS:
            arrive(r, 1)
            start(r, 2)
        r = step - 1
        if 0 <= r < ROUNDS:
            arrive(r, 0)
            start(r, 1)
        if step < ROUNDS:
            wait_own_unit(step)
            start(step, 0)
        r = step - 4
        if 0 <= r < ROUNDS:
            arrive(r, 3)
            first, last = ROUND_GROUPS[r]
            lax.fori_loop(0, first - last + 1, lambda i, c, first=first: group(first - i, c), 0)

    keep = pltpu.make_async_copy(x_ref.at[:, my_cols, :], out_ref.at[row], z_sem.at[0])
    give = pltpu.make_async_remote_copy(
        src_ref=x_ref.at[:, pl.ds(pl.multiple_of(32 * other, 32), 32), :], dst_ref=out_ref.at[row],
        send_sem=z_sem.at[1], recv_sem=z_sem.at[2],
        device_id={"row": other}, device_id_type=MESH_ID)
    keep.start()
    give.start()
    each_block(place_done)
    for r in range(ROUNDS):
        for phase in range(4):
            for c in range(3):
                for h in hops(r, c, phase, False):
                    h.wait_send()
    keep.wait()
    give.wait()


def solution(mesh):
    def local_apply(v_loc, t_loc, z_loc):
        vt = v_loc.reshape(24, 128, 3, 32).transpose(2, 0, 3, 1)
        tp = jnp.concatenate([t_loc.transpose(1, 0, 2).reshape(32, 96), jnp.zeros((32, 32), F32)], axis=1)
        zt = z_loc.reshape(2, 12, 256, 32).transpose(0, 1, 3, 2)
        hbm = pl.BlockSpec(memory_space=pl.ANY)
        out = pl.pallas_call(
            kernel,
            out_shape=jax.ShapeDtypeStruct((2, 12, 32, 256), F32),
            in_specs=[hbm, hbm, hbm],
            out_specs=hbm,
            scratch_shapes=[
                pltpu.VMEM((ROUNDS, 4, 4, 4, 256, 128), F32),
                pltpu.VMEM((12, 64, 256), F32),
                pltpu.VMEM((12, 256, 256), BF16),
                pltpu.VMEM((12, 256, 256), BF16),
                pltpu.VMEM((12, 256, 256), BF16),
                pltpu.VMEM((64, 256), F32),
                pltpu.VMEM((256, 256), F32),
                pltpu.VMEM((256, 256), F32),
                pltpu.VMEM((2, 320, 256), F32),
                pltpu.VMEM((2, 320, 256), F32),
                pltpu.SemaphoreType.DMA((4, 24)),
                pltpu.SemaphoreType.DMA((ROUNDS,)),
                pltpu.SemaphoreType.DMA((3,)),
                pltpu.SemaphoreType.DMA((ROUNDS, 3, 10)),
                pltpu.SemaphoreType.DMA((ROUNDS, 3, 10)),
                pltpu.SemaphoreType.DMA((2,)),
                pltpu.SemaphoreType.DMA((2,)),
            ],
            compiler_params=pltpu.CompilerParams(has_side_effects=True, vmem_limit_bytes=67_000_000),
        )(vt, tp, zt)
        return out.transpose(0, 1, 3, 2).reshape(6144, 32)

    return jax.shard_map(
        local_apply,
        mesh=mesh,
        in_specs=(P("row", "col"), P("col", None, None), P(None, ("row", "col"))),
        out_specs=P(None, ("row", "col")),
        check_vma=False,
    )
```
